64 devices in a mesh: dp: 4 (over x, y), tp: 16 (over z, core).
Axes of the slice: x: 2, y: 2, z: 8, core: 2. Of those that a mesh axis runs over, the one named last changes fastest.
The devices are a block of a 4x4x8 slice.
Arguments:
- hidden: bfloat16 [4, 2048, 2560], P('dp'), parts along dimension 0
- ln_gain: float32 [2560], replicated
- ln_bias: float32 [2560], replicated
- embedding: bfloat16 [51200, 2560], P('tp')
- targets: int32 [4, 2048], P('dp'), parts along dimension 0
- score_mask: int32 [4, 2048], P('dp'), parts along dimension 0
Outputs:
- output 1: float32 [4, 2048], P('dp'), parts along dimension 0
- output 2: float32 [4, 2048], P('dp'), parts along dimension 0
- output 3: float32 [4], P('dp'), parts along dimension 0
- output 4: float32 [4, 2048], P('dp'), parts along dimension 0
There are 4 independent parts. The reference program is written for one: setup_inputs(seed, part) draws one part's arguments, and reference() takes and returns one part's arrays. A program takes and returns all parts, laid end to end along the dimension named above; an argument that names none is the same for every part.
All inputs are finite; a program needn't handle non-finite values.
Results may differ from the reference program's by a relative error of at most 0.001.
Values sent between devices are 32-bit elements.
A program may use at most 768 MiB of HBM per device.

```python
import jax
import jax.numpy as jnp
from jax import lax

BATCH = 1
SEQ_LEN = 2048
D_MODEL = 2560
VOCAB = 50272
VOCAB_PAD = 51200
LN_EPS = 1e-5
LOGIT_SCALE = 3.0


def setup_inputs(seed: int = 0, part: int = 0) -> dict:
    part_key = jax.random.fold_in(jax.random.key(seed), part)
    shared_key = jax.random.key(seed + 1)
    key_x, key_tgt, key_lo, key_hi = jax.random.split(part_key, 4)
    key_g, key_b, key_e = jax.random.split(shared_key, 3)
    hidden = jax.random.normal(key_x, (BATCH, SEQ_LEN, D_MODEL), jnp.float32).astype(jnp.bfloat16)
    ln_gain = 1.0 + 0.3 * jax.random.normal(key_g, (D_MODEL,), jnp.float32)
    ln_bias = 0.5 * jax.random.normal(key_b, (D_MODEL,), jnp.float32)
    embedding = (jax.random.normal(key_e, (VOCAB_PAD, D_MODEL), jnp.float32) * (LOGIT_SCALE * D_MODEL ** -0.5)).astype(jnp.bfloat16)
    targets = jax.random.randint(key_tgt, (BATCH, SEQ_LEN), 0, VOCAB, jnp.int32)
    targets = targets.at[0, 0].set(0).at[0, SEQ_LEN - 1].set(VOCAB - 1)
    positions = jnp.arange(SEQ_LEN)[None, :]
    run_start = jax.random.randint(key_lo, (BATCH, 1), 0, SEQ_LEN // 2, jnp.int32)
    run_stop = jax.random.randint(key_hi, (BATCH, 1), SEQ_LEN // 2 + 1, SEQ_LEN + 1, jnp.int32)
    score_mask = ((positions >= run_start) & (positions < run_stop)).astype(jnp.int32)
    return {"hidden": hidden, "ln_gain": ln_gain, "ln_bias": ln_bias, "embedding": embedding, "targets": targets, "score_mask": score_mask}


def reference(hidden, ln_gain, ln_bias, embedding, targets, score_mask):
    vocab_ids = jnp.arange(VOCAB_PAD)
    valid_rows = vocab_ids < VOCAB

    def score_row(row):
        hidden_row, target_row, mask_row = row
        hidden_f = hidden_row.astype(jnp.float32)
        row_mean = jnp.mean(hidden_f, axis=-1, keepdims=True)
        centered = hidden_f - row_mean
        row_var = jnp.mean(centered * centered, axis=-1, keepdims=True)
        normed = (centered * lax.rsqrt(row_var + LN_EPS) * ln_gain + ln_bias).astype(jnp.bfloat16)
        logits = jnp.dot(normed, embedding.T, preferred_element_type=jnp.float32)
        logits = jnp.where(valid_rows[None, :], logits, -jnp.inf)
        row_max = jnp.max(logits, axis=-1)
        log_norm = row_max + jnp.log(jnp.sum(jnp.exp(logits - row_max[:, None]), axis=-1))
        target_logit = jnp.sum(jnp.where(vocab_ids[None, :] == target_row[:, None], logits, 0.0), axis=-1)
        token_logp = (target_logit - log_norm) * mask_row.astype(jnp.float32)
        return log_norm, token_logp, jnp.sum(token_logp), row_max - log_norm

    log_norm, token_logp, seq_score, top_logp = lax.map(score_row, (hidden, targets, score_mask))
    return log_norm, token_logp, seq_score, top_logp
```

```python
import functools

import jax
import jax.numpy as jnp
from jax import lax
from jax.experimental import pallas as pl
from jax.experimental.pallas import tpu as pltpu
from jax.sharding import PartitionSpec as P

OPT_VOCAB = 50272
LN_EPS = 1e-5
MESH = pl.DeviceIdType.MESH
TILE = 512
LANES = 128
CHUNK = 400
PIECE = 80
LNROWS = 16
LN_PLAN = (6, 6, 6, 5, 5, 4, 0, 0)
E_GROUPS = ((0, 2), (2, 4), (4, 8))


def kernel(n, x_hbm, gain_hbm, bias_hbm, e_hbm, tgt_hbm, mask_hbm, out_ref,
           x_ref, e_ref, h_ref, gain1_ref, bias1_ref, gain_ref, bias_ref, tgt_ref, mask_ref, m_ref, s_ref, t_ref, comm_ref,
           x_sem, e_sem, small_sem, send_sem, recv_sem, *, seq, vocab, depth):
    ntile = seq // TILE
    nchunk = vocab // CHUNK
    me = lax.axis_index("tp")

    def x_copy(b):
        rows = pl.ds(pl.multiple_of(b * TILE, TILE), TILE)
        return pltpu.make_async_copy(x_hbm.at[rows, :], x_ref.at[rows, :], x_sem.at[b])

    def e_copy(g):
        first, last = E_GROUPS[g]
        rows = pl.ds(first * CHUNK, (last - first) * CHUNK)
        return pltpu.make_async_copy(e_hbm.at[rows, :], e_ref.at[rows, :], e_sem.at[g])

    small = [pltpu.make_async_copy(src, dst, small_sem.at[i]) for i, (src, dst) in enumerate(
        ((gain_hbm, gain1_ref), (bias_hbm, bias1_ref), (tgt_hbm, tgt_ref), (mask_hbm, mask_ref)))]
    for copy in small[:2]:
        copy.start()
    x_copy(0).start()
    e_copy(0).start()
    for copy in small[2:]:
        copy.start()
    e_copy(1).start()
    x_copy(1).start()
    e_copy(2).start()
    for b in range(2, ntile):
        x_copy(b).start()

    barrier = pltpu.get_barrier_semaphore()
    for d in range(1, n):
        pl.semaphore_signal(barrier, inc=1, device_id={"tp": lax.rem(me + d, n)}, device_id_type=MESH)

    m_ref[...] = jnp.full_like(m_ref, -jnp.inf)
    s_ref[...] = jnp.zeros_like(s_ref)
    t_ref[...] = jnp.zeros_like(t_ref)
    small[0].wait()
    small[1].wait()
    gain_ref[...] = gain1_ref[...].reshape(1, depth)
    bias_ref[...] = bias1_ref[...].reshape(1, depth)

    def norm_block(row, slot, hrow):
        x = x_ref[pl.ds(row, LNROWS), :].astype(jnp.float32)
        mean = jnp.sum(x, axis=-1, keepdims=True) * (1.0 / depth)
        centered = x - mean
        var = jnp.sum(centered * centered, axis=-1, keepdims=True) * (1.0 / depth)
        y = centered * lax.rsqrt(var + LN_EPS) * gain_ref[...] + bias_ref[...]
        h_ref[slot, pl.ds(hrow, LNROWS), :] = y.astype(jnp.bfloat16)

    x_copy(0).wait()

    def first_norm(j, carry):
        for q in range(8):
            row = pl.multiple_of(j * (8 * LNROWS) + q * LNROWS, LNROWS)
            norm_block(row, 0, row)
        return carry

    lax.fori_loop(0, TILE // (8 * LNROWS), first_norm, 0)
    small[2].wait()
    small[3].wait()

    nvalid = OPT_VOCAB - me * vocab
    sub = lax.broadcasted_iota(jnp.int32, (8, TILE), 0)

    def update(z, tile, base):
        m, total, hit = m_ref[tile], s_ref[tile], t_ref[tile]
        tgt = tgt_ref[0:1, pl.ds(pl.multiple_of(tile * TILE, TILE), TILE)]
        rel = (tgt - me * vocab - base) - sub
        for q in range(0, CHUNK, PIECE):
            v = [z[r:r + 8] for r in range(q, q + PIECE, 8)]
            v = [a + jnp.where(base + q + 8 * j < nvalid, 0.0, -jnp.inf) for j, a in enumerate(v)]
            m_new = functools.reduce(jnp.maximum, v, m)
            total = total * jnp.exp(m - m_new)
            for a in v:
                total += jnp.exp(a - m_new)
            m = m_new
            for j, a in enumerate(v):
                hit = jnp.where(rel == q + 8 * j, a, hit)
        m_ref[tile], s_ref[tile], t_ref[tile] = m, total, hit

    def run_tile(tile, slot, nxt, first):
        blk = 0
        for c in range(nchunk):
            if first:
                for g, (start, _) in enumerate(E_GROUPS):
                    if start == c:
                        e_copy(g).wait()
            e = e_ref[c * CHUNK:(c + 1) * CHUNK, :]
            z = lax.dot_general(e, h_ref[slot], (((1,), (1,)), ((), ())), preferred_element_type=jnp.float32)
            update(z, tile, c * CHUNK)
            for _ in range(LN_PLAN[c]):
                row = blk * LNROWS
                norm_block(pl.multiple_of(nxt * TILE + row, LNROWS), 1 - slot, row)
                blk += 1

    def send(tile, d):
        return pltpu.make_async_remote_copy(
            src_ref=comm_ref.at[tile, me], dst_ref=comm_ref.at[tile, me],
            send_sem=send_sem.at[tile, d], recv_sem=recv_sem.at[tile, d],
            device_id={"tp": lax.rem(me + d, n)}, device_id_type=MESH)

    def finish_tile(tile):
        m = m_ref[tile]
        top = jnp.max(m, axis=0, keepdims=True)
        total = jnp.sum(s_ref[tile] * jnp.exp(m - top), axis=0, keepdims=True)
        hit = jnp.sum(t_ref[tile], axis=0, keepdims=True)
        for g, v in enumerate((top, total, hit)):
            for j in range(TILE // LANES):
                r = g * (TILE // LANES) + j
                comm_ref[tile, me, r:r + 1, :] = v[:, j * LANES:(j + 1) * LANES]
        for d in range(1, n):
            send(tile, d).start()

    x_copy(1).wait()
    run_tile(0, 0, 1, True)
    pl.semaphore_wait(barrier, n - 1)
    finish_tile(0)

    def step(tile, carry):
        @pl.when(tile < ntile - 1)
        def _():
            x_copy(tile + 1).wait()

        run_tile(tile, lax.rem(tile, 2), jnp.minimum(tile + 1, ntile - 1), False)
        finish_tile(tile)
        return carry

    lax.fori_loop(1, ntile, step, 0)

    rows_t = TILE // LANES
    rows_o = seq // LANES
    acc = jnp.zeros((rows_t, LANES), jnp.float32)
    for tile in range(ntile):
        for d in range(1, n):
            send(tile, d).wait_recv()
        tops = [comm_ref[tile, p, 0:rows_t, :] for p in range(n)]
        top = functools.reduce(jnp.maximum, tops)
        total = sum(comm_ref[tile, p, rows_t:2 * rows_t, :] * jnp.exp(tops[p] - top) for p in range(n))
        hit = sum(comm_ref[tile, p, 2 * rows_t:3 * rows_t, :] for p in range(n))
        rows = slice(tile * rows_t, (tile + 1) * rows_t)
        logn = top + jnp.log(total)
        tok = (hit - logn) * mask_ref[rows, :].astype(jnp.float32)
        acc += tok
        for g, v in enumerate((logn, tok, top - logn)):
            out_ref[g * rows_o + tile * rows_t:g * rows_o + (tile + 1) * rows_t, :] = v
    acc = jnp.sum(jnp.sum(acc, axis=0, keepdims=True), axis=1, keepdims=True)
    out_ref[3 * rows_o:3 * rows_o + 8, :] = jnp.broadcast_to(acc, (8, LANES))
    for tile in range(ntile):
        for d in range(1, n):
            send(tile, d).wait_send()


def solution(mesh):
    n = mesh.shape["tp"]

    def local_part(hidden, ln_gain, ln_bias, embedding, targets, score_mask):
        batch, seq, depth = hidden.shape
        vocab = embedding.shape[0]
        ntile = seq // TILE
        rows = seq // LANES
        hbm = pl.BlockSpec(memory_space=pltpu.HBM)
        state = pltpu.VMEM((ntile, 8, TILE), jnp.float32)
        out = pl.pallas_call(
            functools.partial(kernel, n, seq=seq, vocab=vocab, depth=depth),
            out_shape=jax.ShapeDtypeStruct((3 * rows + 8, LANES), jnp.float32),
            in_specs=[hbm] * 6,
            out_specs=pl.BlockSpec(memory_space=pltpu.VMEM),
            scratch_shapes=[
                pltpu.VMEM((seq, depth), jnp.bfloat16),
                pltpu.VMEM((vocab, depth), jnp.bfloat16),
                pltpu.VMEM((2, TILE, depth), jnp.bfloat16),
                pltpu.VMEM((depth,), jnp.float32),
                pltpu.VMEM((depth,), jnp.float32),
                pltpu.VMEM((1, depth), jnp.float32),
                pltpu.VMEM((1, depth), jnp.float32),
                pltpu.VMEM((1, seq), jnp.int32),
                pltpu.VMEM((rows, LANES), jnp.int32),
                state, state, state,
                pltpu.VMEM((ntile, n, 3 * TILE // LANES, LANES), jnp.float32),
                pltpu.SemaphoreType.DMA((ntile,)),
                pltpu.SemaphoreType.DMA((len(E_GROUPS),)),
                pltpu.SemaphoreType.DMA((4,)),
                pltpu.SemaphoreType.DMA((ntile, n)),
                pltpu.SemaphoreType.DMA((ntile, n)),
            ],
            compiler_params=pltpu.CompilerParams(collective_id=0, has_side_effects=True,
                                                 vmem_limit_bytes=61 * 1024 * 1024),
            name="score",
        )(hidden.reshape(batch * seq, depth), ln_gain, ln_bias, embedding,
          targets.reshape(1, seq), score_mask.reshape(rows, LANES))
        logn, tok, top = (out[g * rows:(g + 1) * rows].reshape(1, seq) for g in range(3))
        return logn, tok, out[3 * rows, 0:1], top

    row_spec = P("dp", None)
    return jax.shard_map(local_part, mesh=mesh, in_specs=(P("dp", None, None), P(), P(), P("tp", None), row_spec, row_spec), out_specs=(row_spec, row_spec, P("dp"), row_spec), check_vma=False)
```

```python
import functools

import jax
import jax.numpy as jnp
from jax import lax
from jax.experimental import pallas as pl
from jax.experimental.pallas import tpu as pltpu
from jax.sharding import PartitionSpec as P

OPT_VOCAB = 50272
LN_EPS = 1e-5
MESH = pl.DeviceIdType.MESH
TILE = 512
LANES = 128
CHUNK = 320
PIECE = 80
LG = 256
LNROWS = 16
XROWS = 128
LN_FIRST = (0, 4, 4, 4, 4, 4, 4, 4, 4, 0)
LN_PLAN = (4, 4, 4, 4, 4, 3, 3, 3, 3, 0)
E_GROUPS = ((0, 2), (2, 5), (5, 10))
UNROLL = False


def kernel(n, x_hbm, gain_hbm, bias_hbm, e_hbm, tgt_hbm, mask_hbm, out_ref,
           x_ref, e_ref, h_ref, gain1_ref, bias1_ref, gain_ref, bias_ref, tgt_ref, mask_ref, m_ref, s_ref, t_ref, comm_ref,
           x_sem, e_sem, small_sem, send_sem, recv_sem, *, seq, vocab, depth):
    ntile = seq // TILE
    nchunk = vocab // CHUNK
    nblk = TILE // XROWS
    me = lax.axis_index("tp")
    zero = me - 2 * lax.div(me, 2) - lax.rem(me, 2)

    def x_copy(first, count, sem):
        rows = pl.ds(first, count)
        return pltpu.make_async_copy(x_hbm.at[rows, :], x_ref.at[rows, :], x_sem.at[sem])

    def x_block(b):
        return x_copy(pl.multiple_of(b * XROWS, XROWS), XROWS, b)

    def x_tile(t):
        return x_copy(pl.multiple_of(t * TILE, TILE), TILE, nblk + t)

    def e_copy(g):
        first, last = E_GROUPS[g]
        rows = pl.ds(first * CHUNK, (last - first) * CHUNK)
        return pltpu.make_async_copy(e_hbm.at[rows, :], e_ref.at[rows, :], e_sem.at[g])

    small = [pltpu.make_async_copy(src, dst, small_sem.at[i]) for i, (src, dst) in enumerate(
        ((gain_hbm, gain1_ref), (bias_hbm, bias1_ref), (tgt_hbm, tgt_ref), (mask_hbm, mask_ref)))]
    x_block(0).start()
    for copy in small:
        copy.start()
    for b in range(1, nblk):
        x_block(b).start()
    e_copy(0).start(priority=1)
    e_copy(1).start(priority=1)
    x_tile(1).start(priority=1)
    for g in range(2, len(E_GROUPS)):
        e_copy(g).start(priority=1)
    for t in range(2, ntile):
        x_tile(t).start(priority=1)

    def peer(d):
        return {"tp": jnp.bitwise_xor(me, d)}

    barrier = pltpu.get_barrier_semaphore()
    for d in range(1, n):
        pl.semaphore_signal(barrier, inc=1, device_id=peer(d), device_id_type=MESH)

    m_ref[...] = jnp.full_like(m_ref, -jnp.inf)
    s_ref[...] = jnp.zeros_like(s_ref)
    t_ref[...] = jnp.zeros_like(t_ref)
    small[0].wait()
    small[1].wait()
    gain_ref[...] = gain1_ref[...].reshape(1, depth)
    bias_ref[...] = bias1_ref[...].reshape(1, depth)

    def norm_block(row, slot, hrow):
        x = x_ref[pl.ds(row, LNROWS), :].astype(jnp.float32)
        mean = jnp.sum(x, axis=-1, keepdims=True) * (1.0 / depth)
        centered = x - mean
        var = jnp.sum(centered * centered, axis=-1, keepdims=True) * (1.0 / depth)
        y = centered * lax.rsqrt(var + LN_EPS) * gain_ref[...] + bias_ref[...]
        h_ref[slot, pl.ds(hrow, LNROWS), :] = y.astype(jnp.bfloat16)

    def first_norm(j, carry):
        x_block(j).wait()
        for q in range(0, XROWS, LNROWS):
            row = pl.multiple_of(j * XROWS + q, LNROWS)
            norm_block(row, 0, row)
        return carry

    lax.fori_loop(0, nblk, first_norm, 0)
    small[2].wait()
    small[3].wait()

    nvalid = OPT_VOCAB - me * vocab
    min_valid = OPT_VOCAB - (n - 1) * vocab
    sub = lax.broadcasted_iota(jnp.int32, (8, LG), 0)

    def padded(v, row, base):
        return v if row < min_valid else v + jnp.where(row < nvalid, 0.0, -jnp.inf)

    def update(z, tile, base):
        for u in range(0, TILE, LG):
            cols = slice(u, u + LG)
            m, total, hit = m_ref[tile, :, cols], s_ref[tile, :, cols], t_ref[tile, :, cols]
            tgt = tgt_ref[0:1, pl.ds(pl.multiple_of(tile * TILE + u, LG), LG)]
            rel = (tgt - me * vocab - base) - sub
            for q in range(0, CHUNK, PIECE):
                v = [padded(z[r:r + 8, cols], base + r, base) for r in range(q, q + PIECE, 8)]
                m_new = functools.reduce(jnp.maximum, v, m)
                total = total * jnp.exp(m - m_new)
                for a in v:
                    total += jnp.exp(a - m_new)
                m = m_new
                for j, a in enumerate(v):
                    hit = jnp.where(rel == q + 8 * j, a, hit)
            m_ref[tile, :, cols], s_ref[tile, :, cols], t_ref[tile, :, cols] = m, total, hit

    def run_tile(tile, slot, nxt, first, plan):
        blk = 0
        for c in range(nchunk):
            if first:
                for g, (start, _) in enumerate(E_GROUPS):
                    if start == c:
                        e_copy(g).wait()
                if c == 1:
                    x_tile(1).wait()
            e = e_ref[c * CHUNK:(c + 1) * CHUNK, :]
            z = lax.dot_general(e, h_ref[slot], (((1,), (1,)), ((), ())), preferred_element_type=jnp.float32)
            update(z, tile, c * CHUNK)
            for _ in range(plan[c]):
                row = blk * LNROWS
                norm_block(pl.multiple_of(nxt * TILE + row, LNROWS), 1 - slot, row)
                blk += 1

    def finish_tile(tile):
        m = m_ref[tile]
        top = jnp.max(m, axis=0, keepdims=True)
        total = jnp.sum(s_ref[tile] * jnp.exp(m - top), axis=0, keepdims=True)
        hit = jnp.sum(t_ref[tile], axis=0, keepdims=True)
        for g, v in enumerate((top, total, hit)):
            for j in range(TILE // LANES):
                r = g * (TILE // LANES) + j
                comm_ref[me, tile, r:r + 1, :] = v[:, j * LANES:(j + 1) * LANES]

    rounds = (pl.ds(0, ntile - 1), pl.ds(ntile - 1, 1))

    def send(r, d):
        return pltpu.make_async_remote_copy(
            src_ref=comm_ref.at[me, rounds[r]], dst_ref=comm_ref.at[me, rounds[r]],
            send_sem=send_sem.at[r, d], recv_sem=recv_sem.at[r, d],
            device_id=peer(d), device_id_type=MESH)

    def first_round():
        pl.semaphore_wait(barrier, n - 1)
        for d in range(1, n):
            send(0, d).start()

    run_tile(zero, zero, zero + 1, True, LN_FIRST)
    finish_tile(0)
    if UNROLL:
        for t in range(1, ntile):
            if t == ntile - 1:
                first_round()
            else:
                x_tile(t + 1).wait()
            run_tile(zero + t, zero + t % 2, zero + t + 1, False, LN_PLAN if t < ntile - 1 else (0,) * nchunk)
            finish_tile(t)
    else:
        def step(t, carry):
            @pl.when(t < ntile - 1)
            def _():
                x_tile(t + 1).wait()

            @pl.when(t == ntile - 1)
            def _():
                first_round()

            run_tile(t, lax.rem(t, 2), jnp.minimum(t + 1, ntile - 1), False, LN_PLAN)
            finish_tile(t)
            return carry

        lax.fori_loop(1, ntile, step, 0)
    for d in range(1, n):
        send(1, d).start()

    rows_t = TILE // LANES
    rows_o = seq // LANES

    def combine(tile):
        tops = [comm_ref[p, tile, 0:rows_t, :] for p in range(n)]
        top = functools.reduce(jnp.maximum, tops)
        total = sum(comm_ref[p, tile, rows_t:2 * rows_t, :] * jnp.exp(tops[p] - top) for p in range(n))
        hit = sum(comm_ref[p, tile, 2 * rows_t:3 * rows_t, :] for p in range(n))
        rows = slice(tile * rows_t, (tile + 1) * rows_t)
        logn = top + jnp.log(total)
        tok = (hit - logn) * mask_ref[rows, :].astype(jnp.float32)
        for g, v in enumerate((logn, tok, top - logn)):
            out_ref[g * rows_o + tile * rows_t:g * rows_o + (tile + 1) * rows_t, :] = v

    for d in range(1, n):
        send(0, d).wait_recv()
    for tile in range(ntile - 1):
        combine(tile)
    for d in range(1, n):
        send(0, d).wait_send()
    for d in range(1, n):
        send(1, d).wait_recv()
    combine(ntile - 1)
    for d in range(1, n):
        send(1, d).wait_send()


def solution(mesh):
    n = mesh.shape["tp"]

    def local_part(hidden, ln_gain, ln_bias, embedding, targets, score_mask):
        batch, seq, depth = hidden.shape
        vocab = embedding.shape[0]
        ntile = seq // TILE
        rows = seq // LANES
        hbm = pl.BlockSpec(memory_space=pltpu.HBM)
        state = pltpu.VMEM((ntile, 8, TILE), jnp.float32)
        out = pl.pallas_call(
            functools.partial(kernel, n, seq=seq, vocab=vocab, depth=depth),
            out_shape=pltpu.VMEM((3 * rows, LANES), jnp.float32),
            in_specs=[hbm] * 6,
            out_specs=pl.BlockSpec(memory_space=pltpu.VMEM),
            scratch_shapes=[
                pltpu.VMEM((seq, depth), jnp.bfloat16),
                pltpu.VMEM((vocab, depth), jnp.bfloat16),
                pltpu.VMEM((2, TILE, depth), jnp.bfloat16),
                pltpu.VMEM((depth,), jnp.float32),
                pltpu.VMEM((depth,), jnp.float32),
                pltpu.VMEM((1, depth), jnp.float32),
                pltpu.VMEM((1, depth), jnp.float32),
                pltpu.VMEM((1, seq), jnp.int32),
                pltpu.VMEM((rows, LANES), jnp.int32),
                state, state, state,
                pltpu.VMEM((n, ntile, 3 * TILE // LANES, LANES), jnp.float32),
                pltpu.SemaphoreType.DMA((TILE // XROWS + ntile,)),
                pltpu.SemaphoreType.DMA((len(E_GROUPS),)),
                pltpu.SemaphoreType.DMA((4,)),
                pltpu.SemaphoreType.DMA((2, n)),
                pltpu.SemaphoreType.DMA((2, n)),
            ],
            compiler_params=pltpu.CompilerParams(collective_id=0, has_side_effects=True,
                                                 vmem_limit_bytes=61 * 1024 * 1024),
            name="score",
        )(hidden.reshape(batch * seq, depth), ln_gain, ln_bias, embedding,
          targets.reshape(1, seq), score_mask.reshape(rows, LANES))
        logn, tok, top = (out[g * rows:(g + 1) * rows].reshape(1, seq) for g in range(3))
        return logn, tok, jnp.sum(tok, axis=-1), top

    row_spec = P("dp", None)
    return jax.shard_map(local_part, mesh=mesh, in_specs=(P("dp", None, None), P(), P(), P("tp", None), row_spec, row_spec), out_specs=(row_spec, row_spec, P("dp"), row_spec), check_vma=False)
```
